32 devices in a mesh: row: 8 (over z, core), col: 4 (over y, x).
Axes of the slice: x: 2, y: 2, z: 4, core: 2. Of those that a mesh axis runs over, the one named last changes fastest.
Arguments:
- right_side: float32 [1, 8, 4, 1024], P(None, 'row'), may hold values from -6 to 6
- inverse_t: bfloat16 [1, 8, 1024, 1024], P(None, 'row', 'col'), as said below
- u_factor: bfloat16 [1, 8, 2, 4, 128, 1024], P(None, 'row', None, 'col'), may hold values from -0.25 to 0.25
- v_factor: bfloat16 [1, 8, 2, 4, 128, 1024], P(None, 'row', None, 'col'), may hold values from -0.1875 to 0.1875
- ranks: int32 [1, 8, 2, 4], P(None, 'row', None, 'col'), may hold values from 4 to 128, as said below
Outputs:
- whitened: float32 [1, 8, 4, 1024], P(None, 'row')
- loglik: float32 [1, 8, 4], P(None, 'row')
The draws below stay inside these ranges and needn't reach their ends.
Inputs may be any that keep to these rules, and one draw needn't show every extreme that they name: Tile (i, j) with j < i uses the first ranks of its factor rows. `inverse_t`: upper triangular with a positive diagonal.
All inputs are finite; a program needn't handle non-finite values.
Results may differ from the reference program's by a relative error of at most 0.0085.
Values sent between devices are 32-bit elements; how exact they have to be, the bound alone decides.
A program may use at most 64 MiB of HBM per device.

```python
import math
import jax
import jax.numpy as jnp

NB = 1024
RMAX = 128
NRHS = 4
CYC = 1
SLAB = 8
N_ROW = 8
N_COL = 4


def draw_inverse_t(key, part):
    key_diag, key_off = jax.random.split(jax.random.fold_in(key, 11))
    shape = (CYC, N_ROW, NB, NB)
    diagonal = jnp.exp(jax.random.uniform(key_diag, (CYC, N_ROW, NB), jnp.float32, math.log(0.3), math.log(1.2)))
    spread = jax.random.normal(key_off, shape, jnp.float32)
    upper = jnp.triu(spread * (0.3 / math.sqrt(NB)), 1)
    eye = jnp.eye(NB, dtype=jnp.float32)
    matrix = upper + eye[None, None, :, :] * diagonal[:, :, :, None]
    return matrix.astype(jnp.bfloat16)


def draw_ranks(key, part):
    slab = CYC * N_ROW
    tile_cols = slab // N_COL
    shape = (CYC, N_ROW, tile_cols, N_COL)
    row_ids = jnp.arange(CYC, dtype=jnp.int32)[:, None, None, None] * N_ROW + jnp.arange(N_ROW, dtype=jnp.int32)[None, :, None, None]
    col_ids = jnp.arange(tile_cols, dtype=jnp.int32)[None, None, :, None] * N_COL + jnp.arange(N_COL, dtype=jnp.int32)[None, None, None, :]
    distance = jnp.maximum(row_ids - col_ids, 1)
    lowest = max(RMAX // 32, 1)
    highest = jnp.maximum(RMAX // distance, lowest)
    raw = jax.random.randint(jax.random.fold_in(key, 23), shape, 0, 1 << 20)
    values = lowest + raw % (highest - lowest + 1)
    forced = (row_ids == 1) & (col_ids == 0)
    values = jnp.where(forced, RMAX, values)
    return values.astype(jnp.int32)


def levels(rng, extent, shards, least, top_value):
    def one(position, parts):
        heights = jax.random.uniform(jax.random.fold_in(jax.random.fold_in(rng, 6), position), (parts,), jnp.float32, least / len(shards), top_value / len(shards))
        return jnp.repeat(jnp.exp(heights), extent[position] // parts).reshape((-1,) + (1,) * (len(extent) - position - 1))

    level = one(*shards[0])
    for cut in shards[1:]:
        level = level * one(*cut)
    return level


def scatter_about(own_key, dims, scale, bound, cuts=(), kind=jnp.bfloat16):
    loudness = levels(own_key, dims, cuts, -0.22, 0.18) if cuts else 1.0
    drawn = jax.random.normal(own_key, dims, jnp.float32) * scale * loudness
    return jnp.minimum(jnp.maximum(drawn, -bound), bound).astype(kind)


def setup_inputs(seed: int = 0) -> dict:
    key_of = jax.random.split(jax.random.key(seed), 6)
    return {
        "right_side": scatter_about(key_of[0], (CYC, N_ROW, NRHS, NB), 1.0, 6.0, ((1, 8),), jnp.float32),
        "inverse_t": draw_inverse_t(jax.random.fold_in(key_of[5], 71), 0),
        "u_factor": scatter_about(key_of[2], (CYC, N_ROW, SLAB // N_COL, N_COL, RMAX, NB), (4 * RMAX) ** -0.5, 0.25, ((1, 8), (3, 4))),
        "v_factor": scatter_about(key_of[3], (CYC, N_ROW, SLAB // N_COL, N_COL, RMAX, NB), NB ** -0.5, 0.1875, ((1, 8), (3, 4))),
        "ranks": draw_ranks(jax.random.fold_in(key_of[5], 71), 0),
    }


def reference(right_side, inverse_t, u_factor, v_factor, ranks):
    slab = CYC * N_ROW
    sources = right_side.reshape(slab, NRHS, NB)
    inverse = inverse_t.reshape(slab, NB, NB)
    u_tiles = u_factor.reshape(slab, slab, RMAX, NB)
    v_tiles = v_factor.reshape(slab, slab, RMAX, NB)
    limits = ranks.reshape(slab, slab)
    rank_index = jnp.arange(RMAX, dtype=jnp.int32)
    tile_index = jnp.arange(slab, dtype=jnp.int32)
    solved = jnp.zeros((slab, NRHS, NB), jnp.float32)
    for row in range(slab):
        rounded = solved.astype(jnp.bfloat16).astype(jnp.float32)
        inner = jnp.einsum('jrn,jkn->jrk', v_tiles[row].astype(jnp.float32), rounded)
        keep = (rank_index[None, :] < limits[row][:, None]) & (tile_index < row)[:, None]
        inner = jnp.where(keep[:, :, None], inner, 0.0).astype(jnp.bfloat16)
        partial_value = jnp.einsum('jrk,jrn->kn', inner.astype(jnp.float32), u_tiles[row].astype(jnp.float32))
        reduced = (sources[row] - partial_value).astype(jnp.bfloat16)
        result = jnp.dot(reduced, inverse[row], preferred_element_type=jnp.float32)
        solved = solved.at[row].set(result)
    diagonal = jnp.diagonal(inverse, axis1=1, axis2=2).astype(jnp.float32)
    logdiag = jnp.mean(jnp.log(diagonal), axis=1)
    quadratic = jnp.mean(solved * solved, axis=2)
    loglik = -0.5 * quadratic + logdiag[:, None] - 0.5 * math.log(2.0 * math.pi)
    return solved.reshape(CYC, N_ROW, NRHS, NB), loglik.reshape(CYC, N_ROW, NRHS)
```

```python
import functools
import math

import jax
import jax.numpy as jnp
from jax import lax
from jax.experimental import pallas as pl
from jax.experimental.pallas import tpu as pltpu
from jax.sharding import PartitionSpec as P

MESH = pl.DeviceIdType.MESH
NT = (((1,), (1,)), ((), ()))


def remote(src, dst, send_sem, recv_sem, device):
    return pltpu.make_async_remote_copy(
        src_ref=src,
        dst_ref=dst,
        send_sem=send_sem,
        recv_sem=recv_sem,
        device_id=device,
        device_id_type=MESH,
    )


def kernel(
    n_row, n_col,
    rhs_ref, inv_ref, u_ref, v_ref, rank_ref,
    white_ref, lik_ref,
    y_in, p_out, p_in, y_row, logs, base,
    y_send, y_recv, p_send, p_recv, o_send, o_recv, l_send, l_recv,
):
    row = lax.axis_index("row")
    col = lax.axis_index("col")
    per_col = u_ref.shape[2]
    rank_max = u_ref.shape[4]
    nrhs, width = rhs_ref.shape[2], rhs_ref.shape[3]
    piece = width // n_col
    peers = [lax.rem(col + k, n_col) for k in range(1, n_col)]
    own_slot = row // n_col
    own_home = lax.rem(row, n_col)

    barrier = pltpu.get_barrier_semaphore()
    for peer in peers:
        pl.semaphore_signal(barrier, inc=1, device_id=(row, peer), device_id_type=MESH)

    def greet_later(i, count):
        pl.semaphore_signal(barrier, inc=1, device_id=(i, own_home), device_id_type=MESH)
        return count + 1

    greeted = lax.fori_loop(row + 1, n_row, greet_later, n_col - 1)
    for q in range(per_col):
        j = q * n_col + col

        @pl.when(j < row)
        def _():
            for s in range(n_col):
                pl.semaphore_signal(barrier, inc=1, device_id=(j, s), device_id_type=MESH)

        greeted = greeted + jnp.where(j < row, n_col, 0)

    for cc in range(n_col):

        @pl.when(col == cc)
        def _():
            lo = cc * piece
            base[...] = rhs_ref[0, 0, :, lo:lo + piece]
            block = inv_ref[0, 0, :, lo:lo + piece].astype(jnp.float32)
            r_id = lax.broadcasted_iota(jnp.int32, (piece, piece), 0)
            c_id = lax.broadcasted_iota(jnp.int32, (piece, piece), 1)
            diagonal = jnp.sum(jnp.where(r_id == c_id, block, 0.0), axis=0, keepdims=True)
            total = jnp.sum(jnp.log(diagonal), axis=1, keepdims=True)
            logs[cc] = jnp.broadcast_to(total, (1, 128))

    pl.semaphore_wait(barrier, greeted)

    for k, peer in enumerate(peers):
        remote(logs.at[col], logs.at[col], l_send.at[k], l_recv.at[col], (row, peer)).start()

    for q in range(per_col):
        j = q * n_col + col

        @pl.when(j < row)
        def _():
            for s in range(n_col):
                remote(y_in.at[q, s], y_in.at[q, s], y_send.at[0], y_recv.at[q, s], (j, s)).wait_recv()
            y = y_in[q, 0]
            for s in range(1, n_col):
                y = y + y_in[q, s]
            inner = lax.dot_general(y.astype(jnp.bfloat16), v_ref[0, 0, q, 0], NT, preferred_element_type=jnp.float32)
            keep = lax.broadcasted_iota(jnp.int32, (nrhs, rank_max), 1) < rank_ref[0, 0, q, 0]
            inner = jnp.where(keep, inner, 0.0).astype(jnp.bfloat16)
            p = jnp.dot(inner, u_ref[0, 0, q, 0], preferred_element_type=jnp.float32)
            for s in range(n_col):
                p_out[q, s] = p[:, s * piece:(s + 1) * piece]
            for k, peer in enumerate(peers):
                remote(p_out.at[q, peer], p_in.at[j], p_send.at[q, k], p_recv.at[j], (row, peer)).start()
            p_in[j] = p_out[q, col]

    def gather_p(j, acc):
        home = lax.rem(j, n_col)

        @pl.when(home != col)
        def _():
            remote(p_in.at[j], p_in.at[j], p_send.at[0, 0], p_recv.at[j], (row, home)).wait_recv()

        return acc + p_in[j]

    total = lax.fori_loop(0, row, gather_p, jnp.zeros((nrhs, piece), jnp.float32))
    reduced = (base[...] - total).astype(jnp.bfloat16)
    y_row[col] = jnp.dot(reduced, inv_ref[0, 0], preferred_element_type=jnp.float32)

    def send_y(i, carry):
        remote(y_row.at[col], y_in.at[own_slot, col], y_send.at[i], y_recv.at[own_slot, col], (i, own_home)).start()
        return carry

    lax.fori_loop(row + 1, n_row, send_y, 0)
    for k, peer in enumerate(peers):
        remote(y_row.at[col], y_row.at[col], o_send.at[k], o_recv.at[col], (row, peer)).start()
    for k, peer in enumerate(peers):
        remote(logs.at[peer], logs.at[peer], l_send.at[k], l_recv.at[peer], (row, peer)).wait_recv()
        remote(y_row.at[peer], y_row.at[peer], o_send.at[k], o_recv.at[peer], (row, peer)).wait_recv()
    y = y_row[0]
    log_sum = logs[0]
    for s in range(1, n_col):
        y = y + y_row[s]
        log_sum = log_sum + logs[s]
    white_ref[0, 0] = y
    quadratic = jnp.sum(y * y, axis=1, keepdims=True) * (1.0 / width)
    lik = -0.5 * quadratic + log_sum * (1.0 / width) - 0.5 * math.log(2.0 * math.pi)
    r_id = lax.broadcasted_iota(jnp.int32, (nrhs, 128), 0)
    c_id = lax.broadcasted_iota(jnp.int32, (nrhs, 128), 1)
    flat = jnp.sum(jnp.where(r_id == c_id, lik, 0.0), axis=0, keepdims=True)
    lik_ref[0] = flat[:, :nrhs]

    def left_y(i, carry):
        remote(y_row.at[col], y_in.at[own_slot, col], y_send.at[i], y_recv.at[own_slot, col], (i, own_home)).wait_send()
        return carry

    lax.fori_loop(row + 1, n_row, left_y, 0)
    for k, peer in enumerate(peers):
        remote(logs.at[col], logs.at[col], l_send.at[k], l_recv.at[col], (row, peer)).wait_send()
        remote(y_row.at[col], y_row.at[col], o_send.at[k], o_recv.at[col], (row, peer)).wait_send()
    for q in range(per_col):
        j = q * n_col + col

        @pl.when(j < row)
        def _():
            for k, peer in enumerate(peers):
                remote(p_out.at[q, peer], p_in.at[j], p_send.at[q, k], p_recv.at[j], (row, peer)).wait_send()


def local(n_row, n_col, right_side, inverse_t, u_factor, v_factor, ranks):
    nrhs, width = right_side.shape[2:]
    per_col = u_factor.shape[2]
    piece = width // n_col
    vmem = pl.BlockSpec(memory_space=pltpu.VMEM)
    dma = pltpu.SemaphoreType.DMA
    return pl.pallas_call(
        functools.partial(kernel, n_row, n_col),
        out_shape=(
            jax.ShapeDtypeStruct((1, 1, nrhs, width), jnp.float32),
            jax.ShapeDtypeStruct((1, 1, nrhs), jnp.float32),
        ),
        in_specs=[vmem, vmem, vmem, vmem, pl.BlockSpec(memory_space=pltpu.SMEM)],
        out_specs=(vmem, vmem),
        scratch_shapes=[
            pltpu.VMEM((per_col, n_col, nrhs, width), jnp.float32),
            pltpu.VMEM((per_col, n_col, nrhs, piece), jnp.float32),
            pltpu.VMEM((n_row, nrhs, piece), jnp.float32),
            pltpu.VMEM((n_col, nrhs, width), jnp.float32),
            pltpu.VMEM((n_col, 1, 128), jnp.float32),
            pltpu.VMEM((nrhs, piece), jnp.float32),
            dma((n_row,)),
            dma((per_col, n_col)),
            dma((per_col, n_col)),
            dma((n_row,)),
            dma((n_col,)),
            dma((n_col,)),
            dma((n_col,)),
            dma((n_col,)),
        ],
        compiler_params=pltpu.CompilerParams(collective_id=0, has_side_effects=True),
        name="forward_solve",
    )(right_side, inverse_t, u_factor, v_factor, ranks)


def solution(mesh):
    placed = (
        P(None, "row", None, None),
        P(None, "row", "col", None),
        P(None, "row", None, "col", None, None),
        P(None, "row", None, "col", None, None),
        P(None, "row", None, "col"),
    )
    return jax.shard_map(
        functools.partial(local, mesh.shape["row"], mesh.shape["col"]),
        mesh=mesh,
        in_specs=placed,
        out_specs=(P(None, "row", None, None), P(None, "row", None)),
        check_vma=False,
    )
```

```python
import functools
import math

import jax
import jax.numpy as jnp
from jax import lax
from jax.experimental import pallas as pl
from jax.experimental.pallas import tpu as pltpu
from jax.sharding import PartitionSpec as P

MESH = pl.DeviceIdType.MESH
NT = (((1,), (1,)), ((), ()))


def remote(src, dst, send_sem, recv_sem, device):
    return pltpu.make_async_remote_copy(
        src_ref=src,
        dst_ref=dst,
        send_sem=send_sem,
        recv_sem=recv_sem,
        device_id=device,
        device_id_type=MESH,
    )


def kernel(
    n_row, n_col,
    rhs_hbm, inv_hbm, u_hbm, v_hbm, rank_ref,
    white_ref, lik_ref,
    rhs_ref, inv_ref, u_ref, v_ref,
    y_in, p_out, p_in, y_row, logs, base,
    v_out, v_in, u_out, u_in, fold, w_out, w_in,
    in_sem, y_send, y_recv, p_send, p_recv, o_send, o_recv, l_send, l_recv,
    v_send, v_recv, u_send, u_recv, w_send, w_recv,
):
    row = lax.axis_index("row")
    col = lax.axis_index("col")
    per_col, rank_max, width = u_ref.shape
    nrhs = rhs_ref.shape[0]
    piece = width // n_col
    peers = [lax.rem(col + k, n_col) for k in range(1, n_col)]
    own_slot = row // n_col
    own_home = lax.rem(row, n_col)
    last = n_row - 1

    copies = [
        pltpu.make_async_copy(v_hbm.at[0, 0, :, 0], v_ref, in_sem.at[0]),
        pltpu.make_async_copy(u_hbm.at[0, 0, :, 0], u_ref, in_sem.at[1]),
        pltpu.make_async_copy(inv_hbm.at[0, 0], inv_ref, in_sem.at[2]),
        pltpu.make_async_copy(rhs_hbm.at[0, 0], rhs_ref, in_sem.at[3]),
    ]
    for copy in copies:
        copy.start()

    short = row >= 2
    feeds = (row >= 1) & (row < last)
    long_count = jnp.where(short, row - 1, row)
    long_first = jnp.where(row == 0, 1, row + 2)

    barrier = pltpu.get_barrier_semaphore()

    def greet(i, s):
        pl.semaphore_signal(barrier, inc=1, device_id=(i, s), device_id_type=MESH)

    for peer in peers:
        greet(row, peer)
    greeted = jnp.int32(n_col - 1)

    @pl.when(row < last)
    def _():
        for s in range(n_col):
            greet(row + 1, s)

    greeted = greeted + jnp.where(row < last, n_col, 0)

    @pl.when(row > 0)
    def _():
        for s in range(n_col):
            greet(row - 1, s)

    greeted = greeted + jnp.where(row > 0, n_col, 0)

    def greet_later(i, count):
        greet(i, own_home)
        return count + 1

    greeted = lax.fori_loop(row + 2, n_row, greet_later, greeted)
    for q in range(per_col):
        j = q * n_col + col

        @pl.when(j < row - 1)
        def _():
            for s in range(n_col):
                greet(j, s)

        greeted = greeted + jnp.where(j < row - 1, n_col, 0)

    prev_slot = jnp.maximum(row - 1, 0) // n_col
    prev_home = lax.rem(jnp.maximum(row - 1, 0), n_col)
    gives = short & (col == prev_home)
    copies[0].wait()
    copies[1].wait()

    @pl.when(gives)
    def _():
        v_tile = v_ref[prev_slot].astype(jnp.float32)
        keep = lax.broadcasted_iota(jnp.int32, (rank_max, width), 0) < rank_ref[prev_slot]
        u_tile = jnp.where(keep, u_ref[prev_slot].astype(jnp.float32), 0.0)
        for s in range(n_col):
            v_out[s] = v_tile[:, s * piece:(s + 1) * piece]
            u_out[s] = u_tile[:, s * piece:(s + 1) * piece]

    pl.semaphore_wait(barrier, greeted)

    def v_copy(s, i):
        part = pl.ds(s, n_col - s)
        return remote(v_out.at[part], v_in.at[part], v_send.at[s], v_recv, (i, s))

    def u_copy(k, peer):
        return remote(u_out.at[peer], u_in, u_send.at[k], u_recv, (row, peer))

    @pl.when(gives)
    def _():
        for s in range(n_col):
            v_copy(s, row - 1).start()
        for k, peer in enumerate(peers):
            u_copy(k, peer).start()
        u_in[...] = u_out[col]

    copies[2].wait()
    copies[3].wait()

    for cc in range(n_col):

        @pl.when(col == cc)
        def _():
            base[...] = rhs_ref[:, cc * piece:(cc + 1) * piece]

    def log_part():
        for cc in range(n_col):

            @pl.when(col == cc)
            def _():
                block = inv_ref[:, cc * piece:(cc + 1) * piece].astype(jnp.float32)
                r_id = lax.broadcasted_iota(jnp.int32, (piece, piece), 0)
                c_id = lax.broadcasted_iota(jnp.int32, (piece, piece), 1)
                diagonal = jnp.sum(jnp.where(r_id == c_id, block, 0.0), axis=0, keepdims=True)
                total = jnp.sum(jnp.log(diagonal), axis=1, keepdims=True)
                logs[cc] = jnp.broadcast_to(total, (1, 128))

        for k, peer in enumerate(peers):
            remote(logs.at[col], logs.at[col], l_send.at[k], l_recv.at[col], (row, peer)).start()

    pl.when(row > 0)(log_part)

    for q in range(per_col):
        j = q * n_col + col

        @pl.when(j < long_count)
        def _():
            for s in range(n_col):
                remote(y_in.at[q, s], y_in.at[q, s], y_send.at[0], y_recv.at[q, s], (j, s)).wait_recv()
            y = y_in[q, 0]
            for s in range(1, n_col):
                y = y + y_in[q, s]
            inner = lax.dot_general(y.astype(jnp.bfloat16), v_ref[q], NT, preferred_element_type=jnp.float32)
            keep = lax.broadcasted_iota(jnp.int32, (nrhs, rank_max), 1) < rank_ref[q]
            inner = jnp.where(keep, inner, 0.0).astype(jnp.bfloat16)
            p = jnp.dot(inner, u_ref[q], preferred_element_type=jnp.float32)
            for s in range(n_col):
                p_out[q, s] = p[:, s * piece:(s + 1) * piece]
            for k, peer in enumerate(peers):
                remote(p_out.at[q, peer], p_in.at[j], p_send.at[q, k], p_recv.at[j], (row, peer)).start()
            p_in[j] = p_out[q, col]

    @pl.when(feeds)
    def _():
        fold[...] = jnp.zeros_like(fold)
        for cc in range(n_col):

            @pl.when(col == cc)
            def _():
                v_copy(cc, row).wait_recv()

        for cc in range(n_col):

            @pl.when(col <= cc)
            def _():
                part = lax.dot_general(
                    inv_ref[:, cc * piece:(cc + 1) * piece],
                    v_in[cc].astype(jnp.bfloat16),
                    NT,
                    preferred_element_type=jnp.float32,
                )
                fold[...] += part

    def gather_p(j, acc):
        home = lax.rem(j, n_col)

        @pl.when(home != col)
        def _():
            remote(p_in.at[j], p_in.at[j], p_send.at[0, 0], p_recv.at[j], (row, home)).wait_recv()

        return acc - p_in[j]

    base[...] = lax.fori_loop(0, long_count, gather_p, base[...])

    @pl.when(short)
    def _():
        @pl.when(col != prev_home)
        def _():
            remote(u_in, u_in, u_send.at[0], u_recv, (row, prev_home)).wait_recv()

        u_part = u_in[...].astype(jnp.bfloat16)
        for s in range(n_col):
            remote(w_in.at[s], w_in.at[s], w_send.at[0], w_recv.at[s], (row - 1, s)).wait_recv()
        inner = w_in[0]
        for s in range(1, n_col):
            inner = inner + w_in[s]
        base[...] -= jnp.dot(inner.astype(jnp.bfloat16), u_part, preferred_element_type=jnp.float32)

    reduced = base[...].astype(jnp.bfloat16)

    @pl.when(feeds)
    def _():
        w_out[...] = jnp.dot(reduced, fold[...].astype(jnp.bfloat16), preferred_element_type=jnp.float32)
        for s in range(n_col):
            remote(w_out, w_in.at[col], w_send.at[s], w_recv.at[col], (row + 1, s)).start()

    y_row[col] = jnp.dot(reduced, inv_ref[...], preferred_element_type=jnp.float32)

    def send_y(i, carry):
        remote(y_row.at[col], y_in.at[own_slot, col], y_send.at[i], y_recv.at[own_slot, col], (i, own_home)).start()
        return carry

    lax.fori_loop(long_first, n_row, send_y, 0)
    for k, peer in enumerate(peers):
        remote(y_row.at[col], y_row.at[col], o_send.at[k], o_recv.at[col], (row, peer)).start()
    pl.when(row == 0)(log_part)
    for k, peer in enumerate(peers):
        remote(logs.at[peer], logs.at[peer], l_send.at[k], l_recv.at[peer], (row, peer)).wait_recv()
        remote(y_row.at[peer], y_row.at[peer], o_send.at[k], o_recv.at[peer], (row, peer)).wait_recv()
    y = y_row[0]
    log_sum = logs[0]
    for s in range(1, n_col):
        y = y + y_row[s]
        log_sum = log_sum + logs[s]
    white_ref[0, 0] = y
    quadratic = jnp.sum(y * y, axis=1, keepdims=True) * (1.0 / width)
    lik = -0.5 * quadratic + log_sum * (1.0 / width) - 0.5 * math.log(2.0 * math.pi)
    r_id = lax.broadcasted_iota(jnp.int32, (nrhs, 128), 0)
    c_id = lax.broadcasted_iota(jnp.int32, (nrhs, 128), 1)
    flat = jnp.sum(jnp.where(r_id == c_id, lik, 0.0), axis=0, keepdims=True)
    lik_ref[0] = flat[:, :nrhs]

    def left_y(i, carry):
        remote(y_row.at[col], y_in.at[own_slot, col], y_send.at[i], y_recv.at[own_slot, col], (i, own_home)).wait_send()
        return carry

    lax.fori_loop(long_first, n_row, left_y, 0)
    for k, peer in enumerate(peers):
        remote(logs.at[col], logs.at[col], l_send.at[k], l_recv.at[col], (row, peer)).wait_send()
        remote(y_row.at[col], y_row.at[col], o_send.at[k], o_recv.at[col], (row, peer)).wait_send()

    @pl.when(feeds)
    def _():
        for s in range(n_col):
            remote(w_out, w_in.at[col], w_send.at[s], w_recv.at[col], (row + 1, s)).wait_send()

    @pl.when(gives)
    def _():
        for s in range(n_col):
            v_copy(s, row - 1).wait_send()
        for k, peer in enumerate(peers):
            u_copy(k, peer).wait_send()

    for q in range(per_col):
        j = q * n_col + col

        @pl.when(j < long_count)
        def _():
            for k, peer in enumerate(peers):
                remote(p_out.at[q, peer], p_in.at[j], p_send.at[q, k], p_recv.at[j], (row, peer)).wait_send()


def local(n_row, n_col, right_side, inverse_t, u_factor, v_factor, ranks):
    nrhs, width = right_side.shape[2:]
    per_col, _, rank_max = u_factor.shape[2:5]
    piece = width // n_col
    vmem = pl.BlockSpec(memory_space=pltpu.VMEM)
    hbm = pl.BlockSpec(memory_space=pl.ANY)
    dma = pltpu.SemaphoreType.DMA

    def f32(*shape):
        return pltpu.VMEM(shape, jnp.float32)

    def bf16(*shape):
        return pltpu.VMEM(shape, jnp.bfloat16)

    return pl.pallas_call(
        functools.partial(kernel, n_row, n_col),
        out_shape=(
            jax.ShapeDtypeStruct((1, 1, nrhs, width), jnp.float32),
            jax.ShapeDtypeStruct((1, 1, nrhs), jnp.float32),
        ),
        in_specs=[hbm, hbm, hbm, hbm, pl.BlockSpec(memory_space=pltpu.SMEM)],
        out_specs=(vmem, vmem),
        scratch_shapes=[
            f32(nrhs, width),
            bf16(piece, width),
            bf16(per_col, rank_max, width),
            bf16(per_col, rank_max, width),
            f32(per_col, n_col, nrhs, width),
            f32(per_col, n_col, nrhs, piece),
            f32(n_row, nrhs, piece),
            f32(n_col, nrhs, width),
            f32(n_col, 1, 128),
            f32(nrhs, piece),
            f32(n_col, rank_max, piece),
            f32(n_col, rank_max, piece),
            f32(n_col, rank_max, piece),
            f32(rank_max, piece),
            f32(piece, rank_max),
            f32(nrhs, rank_max),
            f32(n_col, nrhs, rank_max),
            dma((4,)),
            dma((n_row,)),
            dma((per_col, n_col)),
            dma((per_col, n_col)),
            dma((n_row,)),
            dma((n_col,)),
            dma((n_col,)),
            dma((n_col,)),
            dma((n_col,)),
            dma((n_col,)),
            dma,
            dma((n_col,)),
            dma,
            dma((n_col,)),
            dma((n_col,)),
        ],
        compiler_params=pltpu.CompilerParams(collective_id=0, has_side_effects=True),
        name="forward_solve",
    )(right_side, inverse_t, u_factor, v_factor, ranks.reshape(per_col))


def solution(mesh):
    placed = (
        P(None, "row", None, None),
        P(None, "row", "col", None),
        P(None, "row", None, "col", None, None),
        P(None, "row", None, "col", None, None),
        P(None, "row", None, "col"),
    )
    return jax.shard_map(
        functools.partial(local, mesh.shape["row"], mesh.shape["col"]),
        mesh=mesh,
        in_specs=placed,
        out_specs=(P(None, "row", None, None), P(None, "row", None)),
        check_vma=False,
    )
```

```python
import functools
import math

import jax
import jax.numpy as jnp
from jax import lax
from jax.experimental import pallas as pl
from jax.experimental.pallas import tpu as pltpu
from jax.sharding import PartitionSpec as P

MESH = pl.DeviceIdType.MESH
NT = (((1,), (1,)), ((), ()))
FIRST_SHORT = 3
NEAR = 2


def remote(src, dst, send_sem, recv_sem, device):
    return pltpu.make_async_remote_copy(
        src_ref=src,
        dst_ref=dst,
        send_sem=send_sem,
        recv_sem=recv_sem,
        device_id=device,
        device_id_type=MESH,
    )


def kernel(
    n_row, n_col,
    rhs_hbm, inv_hbm, u_hbm, v_hbm, rank_ref,
    white_ref, lik_ref,
    rhs_ref, inv_ref, u_ref, v_ref,
    y_in, p_out, p_in, y_row, logs, base,
    v_out, v_in, u_out, u_in, fold, w_out, w_in, y_full, y_all,
    in_sem, y_send, y_recv, p_send, p_recv, o_send, o_recv, l_send, l_recv,
    v_send, v_recv, u_send, u_recv, w_send, w_recv,
):
    row = lax.axis_index("row")
    col = lax.axis_index("col")
    per_col, rank_max, width = u_ref.shape
    nrhs = rhs_ref.shape[0]
    piece = width // n_col
    peers = [lax.rem(col + k, n_col) for k in range(1, n_col)]
    own_slot = row // n_col
    own_home = lax.rem(row, n_col)
    last = n_row - 1

    copies = [
        pltpu.make_async_copy(v_hbm.at[0, 0, :, 0], v_ref, in_sem.at[0]),
        pltpu.make_async_copy(u_hbm.at[0, 0, :, 0], u_ref, in_sem.at[1]),
        pltpu.make_async_copy(inv_hbm.at[0, 0], inv_ref, in_sem.at[2]),
        pltpu.make_async_copy(rhs_hbm.at[0, 0], rhs_ref, in_sem.at[3]),
    ]
    for copy in copies:
        copy.start()

    short = row >= FIRST_SHORT
    feeds = (row + 1 >= FIRST_SHORT) & (row < last)
    long_count = jnp.where(short, row - 1, row)
    long_first = jnp.where(feeds, row + 2, row + 1)
    near_end = jnp.minimum(row + NEAR + 1, n_row)
    relays = col == own_home

    barrier = pltpu.get_barrier_semaphore()

    def greet(i, s):
        pl.semaphore_signal(barrier, inc=1, device_id=(i, s), device_id_type=MESH)

    for peer in peers:
        greet(row, peer)
    greeted = jnp.int32(n_col - 1)

    @pl.when(row < last)
    def _():
        for s in range(n_col):
            greet(row + 1, s)

    greeted = greeted + jnp.where(row < last, n_col, 0)

    @pl.when(row > 0)
    def _():
        for s in range(n_col):
            greet(row - 1, s)

    greeted = greeted + jnp.where(row > 0, n_col, 0)

    for d in range(2, NEAR + 1):

        @pl.when(row + d < n_row)
        def _():
            greet(row + d, own_home)

        greeted = greeted + jnp.where(row + d < n_row, 1, 0)
        fed = (row >= d) & (lax.rem(jnp.maximum(row - d, 0), n_col) == col)

        @pl.when(fed)
        def _():
            for s in range(n_col):
                greet(row - d, s)

        greeted = greeted + jnp.where(fed, n_col, 0)

    def greet_far(i, count):
        greet(i, col)
        return count + 1

    greeted = lax.fori_loop(jnp.where(relays, near_end, n_row), n_row, greet_far, greeted)
    for q in range(per_col):
        j = q * n_col + col

        @pl.when(j < row - NEAR)
        def _():
            greet(j, col)

        greeted = greeted + jnp.where(j < row - NEAR, 1, 0)

    prev_slot = jnp.maximum(row - 1, 0) // n_col
    prev_home = lax.rem(jnp.maximum(row - 1, 0), n_col)
    gives = short & (col == prev_home)
    copies[0].wait()
    copies[1].wait()

    @pl.when(gives)
    def _():
        v_tile = v_ref[prev_slot].astype(jnp.float32)
        keep = lax.broadcasted_iota(jnp.int32, (rank_max, width), 0) < rank_ref[prev_slot]
        u_tile = jnp.where(keep, u_ref[prev_slot].astype(jnp.float32), 0.0)
        for s in range(n_col):
            v_out[s] = v_tile[:, s * piece:(s + 1) * piece]
            u_out[s] = u_tile[:, s * piece:(s + 1) * piece]

    pl.semaphore_wait(barrier, greeted)

    def v_copy(s, i):
        part = pl.ds(s, n_col - s)
        return remote(v_out.at[part], v_in.at[part], v_send.at[s], v_recv, (i, s))

    def u_copy(k, peer):
        return remote(u_out.at[peer], u_in, u_send.at[k], u_recv, (row, peer))

    @pl.when(gives)
    def _():
        for s in range(n_col):
            v_copy(s, row - 1).start()
        for k, peer in enumerate(peers):
            u_copy(k, peer).start()
        u_in[...] = u_out[col]

    copies[2].wait()
    copies[3].wait()

    for cc in range(n_col):

        @pl.when(col == cc)
        def _():
            base[...] = rhs_ref[:, cc * piece:(cc + 1) * piece]

    def log_part():
        for cc in range(n_col):

            @pl.when(col == cc)
            def _():
                block = inv_ref[:, cc * piece:(cc + 1) * piece].astype(jnp.float32)
                r_id = lax.broadcasted_iota(jnp.int32, (piece, piece), 0)
                c_id = lax.broadcasted_iota(jnp.int32, (piece, piece), 1)
                diagonal = jnp.sum(jnp.where(r_id == c_id, block, 0.0), axis=0, keepdims=True)
                total = jnp.sum(jnp.log(diagonal), axis=1, keepdims=True)
                logs[cc] = jnp.broadcast_to(total, (1, 128))

        for k, peer in enumerate(peers):
            remote(logs.at[col], logs.at[col], l_send.at[k], l_recv.at[col], (row, peer)).start()

    pl.when(row > 0)(log_part)

    for q in range(per_col):
        j = q * n_col + col

        @pl.when(j < long_count)
        def _():
            near = row - j <= NEAR
            remote(y_in.at[q, 0], y_in.at[q, 0], y_send.at[0], y_recv.at[q, 0], (j, col)).wait_recv()

            @pl.when(near)
            def _():
                for s in range(1, n_col):
                    remote(y_in.at[q, s], y_in.at[q, s], y_send.at[0], y_recv.at[q, s], (j, s)).wait_recv()
                y = y_in[q, 0]
                for s in range(1, n_col):
                    y = y + y_in[q, s]
                y_full[...] = y

            @pl.when(jnp.logical_not(near))
            def _():
                y_full[...] = y_in[q, 0]

            y = y_full[...]
            inner = lax.dot_general(y.astype(jnp.bfloat16), v_ref[q], NT, preferred_element_type=jnp.float32)
            keep = lax.broadcasted_iota(jnp.int32, (nrhs, rank_max), 1) < rank_ref[q]
            inner = jnp.where(keep, inner, 0.0).astype(jnp.bfloat16)
            p = jnp.dot(inner, u_ref[q], preferred_element_type=jnp.float32)
            for s in range(n_col):
                p_out[q, s] = p[:, s * piece:(s + 1) * piece]
            for k, peer in enumerate(peers):
                remote(p_out.at[q, peer], p_in.at[j], p_send.at[q, k], p_recv.at[j], (row, peer)).start()
            p_in[j] = p_out[q, col]

    @pl.when(feeds)
    def _():
        fold[...] = jnp.zeros_like(fold)
        for cc in range(n_col):

            @pl.when(col == cc)
            def _():
                v_copy(cc, row).wait_recv()

        for cc in range(n_col):

            @pl.when(col <= cc)
            def _():
                part = lax.dot_general(
                    inv_ref[:, cc * piece:(cc + 1) * piece],
                    v_in[cc].astype(jnp.bfloat16),
                    NT,
                    preferred_element_type=jnp.float32,
                )
                fold[...] += part

    def gather_p(j, acc):
        home = lax.rem(j, n_col)

        @pl.when(home != col)
        def _():
            remote(p_in.at[j], p_in.at[j], p_send.at[0, 0], p_recv.at[j], (row, home)).wait_recv()

        return acc - p_in[j]

    base[...] = lax.fori_loop(0, long_count, gather_p, base[...])

    @pl.when(short)
    def _():
        @pl.when(col != prev_home)
        def _():
            remote(u_in, u_in, u_send.at[0], u_recv, (row, prev_home)).wait_recv()

        u_part = u_in[...].astype(jnp.bfloat16)
        for s in range(n_col):
            remote(w_in.at[s], w_in.at[s], w_send.at[0], w_recv.at[s], (row - 1, s)).wait_recv()
        inner = w_in[0]
        for s in range(1, n_col):
            inner = inner + w_in[s]
        base[...] -= jnp.dot(inner.astype(jnp.bfloat16), u_part, preferred_element_type=jnp.float32)

    reduced = base[...].astype(jnp.bfloat16)

    @pl.when(feeds)
    def _():
        w_out[...] = jnp.dot(reduced, fold[...].astype(jnp.bfloat16), preferred_element_type=jnp.float32)
        for s in range(n_col):
            remote(w_out, w_in.at[col], w_send.at[s], w_recv.at[col], (row + 1, s)).start()

    y_row[col] = jnp.dot(reduced, inv_ref[...], preferred_element_type=jnp.float32)

    def send_y(i, carry):
        remote(y_row.at[col], y_in.at[own_slot, col], y_send.at[i], y_recv.at[own_slot, col], (i, own_home)).start()
        return carry

    lax.fori_loop(long_first, near_end, send_y, 0)
    for k, peer in enumerate(peers):
        remote(y_row.at[col], y_row.at[col], o_send.at[k], o_recv.at[col], (row, peer)).start()
    pl.when(row == 0)(log_part)
    for k, peer in enumerate(peers):
        remote(logs.at[peer], logs.at[peer], l_send.at[k], l_recv.at[peer], (row, peer)).wait_recv()
        remote(y_row.at[peer], y_row.at[peer], o_send.at[k], o_recv.at[peer], (row, peer)).wait_recv()
    y = y_row[0]
    log_sum = logs[0]
    for s in range(1, n_col):
        y = y + y_row[s]
        log_sum = log_sum + logs[s]
    y_all[...] = y

    def far_copy(i):
        return remote(y_all, y_in.at[own_slot, 0], y_send.at[i], y_recv.at[own_slot, 0], (i, col))

    def send_far(i, carry):
        far_copy(i).start()
        return carry

    lax.fori_loop(jnp.where(relays, near_end, n_row), n_row, send_far, 0)
    white_ref[0, 0] = y
    quadratic = jnp.sum(y * y, axis=1, keepdims=True) * (1.0 / width)
    lik = -0.5 * quadratic + log_sum * (1.0 / width) - 0.5 * math.log(2.0 * math.pi)
    r_id = lax.broadcasted_iota(jnp.int32, (nrhs, 128), 0)
    c_id = lax.broadcasted_iota(jnp.int32, (nrhs, 128), 1)
    flat = jnp.sum(jnp.where(r_id == c_id, lik, 0.0), axis=0, keepdims=True)
    lik_ref[0] = flat[:, :nrhs]

    def left_y(i, carry):
        remote(y_row.at[col], y_in.at[own_slot, col], y_send.at[i], y_recv.at[own_slot, col], (i, own_home)).wait_send()
        return carry

    lax.fori_loop(long_first, near_end, left_y, 0)

    def left_far(i, carry):
        far_copy(i).wait_send()
        return carry

    lax.fori_loop(jnp.where(relays, near_end, n_row), n_row, left_far, 0)
    for k, peer in enumerate(peers):
        remote(logs.at[col], logs.at[col], l_send.at[k], l_recv.at[col], (row, peer)).wait_send()
        remote(y_row.at[col], y_row.at[col], o_send.at[k], o_recv.at[col], (row, peer)).wait_send()

    @pl.when(feeds)
    def _():
        for s in range(n_col):
            remote(w_out, w_in.at[col], w_send.at[s], w_recv.at[col], (row + 1, s)).wait_send()

    @pl.when(gives)
    def _():
        for s in range(n_col):
            v_copy(s, row - 1).wait_send()
        for k, peer in enumerate(peers):
            u_copy(k, peer).wait_send()

    for q in range(per_col):
        j = q * n_col + col

        @pl.when(j < long_count)
        def _():
            for k, peer in enumerate(peers):
                remote(p_out.at[q, peer], p_in.at[j], p_send.at[q, k], p_recv.at[j], (row, peer)).wait_send()


def local(n_row, n_col, right_side, inverse_t, u_factor, v_factor, ranks):
    nrhs, width = right_side.shape[2:]
    per_col, _, rank_max = u_factor.shape[2:5]
    piece = width // n_col
    vmem = pl.BlockSpec(memory_space=pltpu.VMEM)
    hbm = pl.BlockSpec(memory_space=pl.ANY)
    dma = pltpu.SemaphoreType.DMA

    def f32(*shape):
        return pltpu.VMEM(shape, jnp.float32)

    def bf16(*shape):
        return pltpu.VMEM(shape, jnp.bfloat16)

    return pl.pallas_call(
        functools.partial(kernel, n_row, n_col),
        out_shape=(
            pltpu.VMEM((1, 1, nrhs, width), jnp.float32),
            pltpu.VMEM((1, 1, nrhs), jnp.float32),
        ),
        in_specs=[hbm, hbm, hbm, hbm, pl.BlockSpec(memory_space=pltpu.SMEM)],
        out_specs=(vmem, vmem),
        scratch_shapes=[
            f32(nrhs, width),
            bf16(piece, width),
            bf16(per_col, rank_max, width),
            bf16(per_col, rank_max, width),
            f32(per_col, n_col, nrhs, width),
            f32(per_col, n_col, nrhs, piece),
            f32(n_row, nrhs, piece),
            f32(n_col, nrhs, width),
            f32(n_col, 1, 128),
            f32(nrhs, piece),
            f32(n_col, rank_max, piece),
            f32(n_col, rank_max, piece),
            f32(n_col, rank_max, piece),
            f32(rank_max, piece),
            f32(piece, rank_max),
            f32(nrhs, rank_max),
            f32(n_col, nrhs, rank_max),
            f32(nrhs, width),
            f32(nrhs, width),
            dma((4,)),
            dma((n_row,)),
            dma((per_col, n_col)),
            dma((per_col, n_col)),
            dma((n_row,)),
            dma((n_col,)),
            dma((n_col,)),
            dma((n_col,)),
            dma((n_col,)),
            dma((n_col,)),
            dma,
            dma((n_col,)),
            dma,
            dma((n_col,)),
            dma((n_col,)),
        ],
        compiler_params=pltpu.CompilerParams(collective_id=0, has_side_effects=True),
        name="forward_solve",
    )(right_side, inverse_t, u_factor, v_factor, ranks.reshape(per_col))


def solution(mesh):
    placed = (
        P(None, "row", None, None),
        P(None, "row", "col", None),
        P(None, "row", None, "col", None, None),
        P(None, "row", None, "col", None, None),
        P(None, "row", None, "col"),
    )
    return jax.shard_map(
        functools.partial(local, mesh.shape["row"], mesh.shape["col"]),
        mesh=mesh,
        in_specs=placed,
        out_specs=(P(None, "row", None, None), P(None, "row", None)),
        check_vma=False,
    )
```

```python
import functools
import math

import jax
import jax.numpy as jnp
from jax import lax
from jax.experimental import pallas as pl
from jax.experimental.pallas import tpu as pltpu
from jax.sharding import PartitionSpec as P

MESH = pl.DeviceIdType.MESH
NT = (((1,), (1,)), ((), ()))
FIRST_SHORT = 4
NEAR = 2


def remote(src, dst, send_sem, recv_sem, device):
    return pltpu.make_async_remote_copy(
        src_ref=src,
        dst_ref=dst,
        send_sem=send_sem,
        recv_sem=recv_sem,
        device_id=device,
        device_id_type=MESH,
    )


def kernel(
    n_row, n_col,
    rhs_hbm, inv_hbm, u_hbm, v_hbm, rank_ref,
    white_ref, lik_ref,
    rhs_ref, inv_ref, u_ref, v_ref,
    y_in, p_out, p_in, y_row, logs, base,
    v_out, v_in, u_out, u_in, fold, w_out, w_in, y_full, y_all,
    in_sem, y_send, y_recv, p_send, p_recv, o_send, o_recv, l_send, l_recv,
    v_send, v_recv, u_send, u_recv, w_send, w_recv, m_send, m_recv, f_send,
):
    row = lax.axis_index("row")
    col = lax.axis_index("col")
    per_col, rank_max, width = u_ref.shape
    nrhs = rhs_ref.shape[0]
    piece = width // n_col
    peers = [lax.rem(col + k, n_col) for k in range(1, n_col)]
    own_slot = row // n_col
    own_home = lax.rem(row, n_col)
    last = n_row - 1

    copies = [
        pltpu.make_async_copy(v_hbm.at[0, 0, :, 0], v_ref, in_sem.at[0]),
        pltpu.make_async_copy(u_hbm.at[0, 0, :, 0], u_ref, in_sem.at[1]),
        pltpu.make_async_copy(inv_hbm.at[0, 0], inv_ref, in_sem.at[2]),
        pltpu.make_async_copy(rhs_hbm.at[0, 0], rhs_ref, in_sem.at[3]),
    ]
    for copy in copies:
        copy.start()

    short = row >= FIRST_SHORT
    feeds = (row + 1 >= FIRST_SHORT) & (row < last)
    long_count = jnp.where(short, row - 1, row)
    long_first = jnp.where(feeds, row + 2, row + 1)
    near_end = jnp.minimum(row + NEAR + 1, n_row)
    relays = col == own_home

    barrier = pltpu.get_barrier_semaphore()

    def greet(i, s):
        pl.semaphore_signal(barrier, inc=1, device_id=(i, s), device_id_type=MESH)

    for peer in peers:
        greet(row, peer)
    greeted = jnp.int32(n_col - 1)

    @pl.when(row < last)
    def _():
        for s in range(n_col):
            greet(row + 1, s)

    greeted = greeted + jnp.where(row < last, n_col, 0)

    @pl.when(row > 0)
    def _():
        for s in range(n_col):
            greet(row - 1, s)

    greeted = greeted + jnp.where(row > 0, n_col, 0)

    for d in range(2, NEAR + 1):

        @pl.when(row + d < n_row)
        def _():
            greet(row + d, own_home)

        greeted = greeted + jnp.where(row + d < n_row, 1, 0)
        fed = (row >= d) & (lax.rem(jnp.maximum(row - d, 0), n_col) == col)

        @pl.when(fed)
        def _():
            for s in range(n_col):
                greet(row - d, s)

        greeted = greeted + jnp.where(fed, n_col, 0)

    def greet_far(i, count):
        greet(i, col)
        return count + 1

    greeted = lax.fori_loop(jnp.where(relays, near_end, n_row), n_row, greet_far, greeted)
    for q in range(per_col):
        j = q * n_col + col

        @pl.when(j < row - NEAR)
        def _():
            greet(j, col)

        greeted = greeted + jnp.where(j < row - NEAR, 1, 0)

    prev_slot = jnp.maximum(row - 1, 0) // n_col
    prev_home = lax.rem(jnp.maximum(row - 1, 0), n_col)
    gives = short & (col == prev_home)
    copies[0].wait()
    copies[1].wait()

    @pl.when(gives)
    def _():
        v_tile = v_ref[prev_slot].astype(jnp.float32)
        keep = lax.broadcasted_iota(jnp.int32, (rank_max, width), 0) < rank_ref[prev_slot]
        u_tile = jnp.where(keep, u_ref[prev_slot].astype(jnp.float32), 0.0)
        for s in range(n_col):
            v_out[s] = v_tile[:, s * piece:(s + 1) * piece]
            u_out[s] = u_tile[:, s * piece:(s + 1) * piece]

    pl.semaphore_wait(barrier, greeted)

    def v_copy(s, i):
        part = pl.ds(s, n_col - s)
        return remote(v_out.at[part], v_in.at[part], v_send.at[s], v_recv, (i, s))

    def u_copy(k, peer):
        return remote(u_out.at[peer], u_in, u_send.at[k], u_recv, (row, peer))

    crosses = short & (lax.rem(row, 2) == 0)

    def by_way(s):
        return crosses & (prev_home != s) & (prev_home + s != n_col - 1)

    def way_copy(cc, s):
        return remote(v_out.at[cc], v_out.at[cc], m_send.at[s], m_recv.at[cc], (row, s))

    @pl.when(gives)
    def _():
        for s in range(n_col):

            @pl.when(by_way(s))
            def _():
                for cc in range(s, n_col):
                    way_copy(cc, s).start()

            @pl.when(jnp.logical_not(by_way(s)))
            def _():
                v_copy(s, row - 1).start()

        for k, peer in enumerate(peers):
            u_copy(k, peer).start()
        u_in[...] = u_out[col]

    @pl.when(by_way(col))
    def _():
        def forward(cc, carry):
            remote(v_out.at[cc], v_out.at[cc], m_send.at[0], m_recv.at[cc], (row, prev_home)).wait_recv()
            remote(v_out.at[cc], v_in.at[cc], f_send, v_recv, (row - 1, col)).start()
            return carry

        lax.fori_loop(col, n_col, forward, 0)

    copies[2].wait()
    copies[3].wait()

    for cc in range(n_col):

        @pl.when(col == cc)
        def _():
            base[...] = rhs_ref[:, cc * piece:(cc + 1) * piece]

    def log_part():
        for cc in range(n_col):

            @pl.when(col == cc)
            def _():
                block = inv_ref[:, cc * piece:(cc + 1) * piece].astype(jnp.float32)
                r_id = lax.broadcasted_iota(jnp.int32, (piece, piece), 0)
                c_id = lax.broadcasted_iota(jnp.int32, (piece, piece), 1)
                diagonal = jnp.sum(jnp.where(r_id == c_id, block, 0.0), axis=0, keepdims=True)
                total = jnp.sum(jnp.log(diagonal), axis=1, keepdims=True)
                logs[cc] = jnp.broadcast_to(total, (1, 128))

        for k, peer in enumerate(peers):
            remote(logs.at[col], logs.at[col], l_send.at[k], l_recv.at[col], (row, peer)).start()

    pl.when(row > 0)(log_part)

    for q in range(per_col):
        j = q * n_col + col

        @pl.when(j < long_count)
        def _():
            near = row - j <= NEAR
            remote(y_in.at[q, 0], y_in.at[q, 0], y_send.at[0], y_recv.at[q, 0], (j, col)).wait_recv()

            @pl.when(near)
            def _():
                for s in range(1, n_col):
                    remote(y_in.at[q, s], y_in.at[q, s], y_send.at[0], y_recv.at[q, s], (j, s)).wait_recv()
                y = y_in[q, 0]
                for s in range(1, n_col):
                    y = y + y_in[q, s]
                y_full[...] = y

            @pl.when(jnp.logical_not(near))
            def _():
                y_full[...] = y_in[q, 0]

            y = y_full[...]
            inner = lax.dot_general(y.astype(jnp.bfloat16), v_ref[q], NT, preferred_element_type=jnp.float32)
            keep = lax.broadcasted_iota(jnp.int32, (nrhs, rank_max), 1) < rank_ref[q]
            inner = jnp.where(keep, inner, 0.0).astype(jnp.bfloat16)
            p = jnp.dot(inner, u_ref[q], preferred_element_type=jnp.float32)
            for s in range(n_col):
                p_out[q, s] = p[:, s * piece:(s + 1) * piece]
            for k, peer in enumerate(peers):
                remote(p_out.at[q, peer], p_in.at[j], p_send.at[q, k], p_recv.at[j], (row, peer)).start()
            p_in[j] = p_out[q, col]

    @pl.when(feeds)
    def _():
        fold[...] = jnp.zeros_like(fold)
        for cc in range(n_col):

            @pl.when(col == cc)
            def _():
                v_copy(cc, row).wait_recv()

        for cc in range(n_col):

            @pl.when(col <= cc)
            def _():
                part = lax.dot_general(
                    inv_ref[:, cc * piece:(cc + 1) * piece],
                    v_in[cc].astype(jnp.bfloat16),
                    NT,
                    preferred_element_type=jnp.float32,
                )
                fold[...] += part

    def gather_p(j, acc):
        home = lax.rem(j, n_col)

        @pl.when(home != col)
        def _():
            remote(p_in.at[j], p_in.at[j], p_send.at[0, 0], p_recv.at[j], (row, home)).wait_recv()

        return acc - p_in[j]

    base[...] = lax.fori_loop(0, long_count, gather_p, base[...])

    @pl.when(short)
    def _():
        @pl.when(col != prev_home)
        def _():
            remote(u_in, u_in, u_send.at[0], u_recv, (row, prev_home)).wait_recv()

        u_part = u_in[...].astype(jnp.bfloat16)
        for s in range(n_col):
            remote(w_in.at[s], w_in.at[s], w_send.at[0], w_recv.at[s], (row - 1, s)).wait_recv()
        inner = w_in[0]
        for s in range(1, n_col):
            inner = inner + w_in[s]
        base[...] -= jnp.dot(inner.astype(jnp.bfloat16), u_part, preferred_element_type=jnp.float32)

    reduced = base[...].astype(jnp.bfloat16)

    @pl.when(feeds)
    def _():
        w_out[...] = jnp.dot(reduced, fold[...].astype(jnp.bfloat16), preferred_element_type=jnp.float32)
        for s in range(n_col):
            remote(w_out, w_in.at[col], w_send.at[s], w_recv.at[col], (row + 1, s)).start()

    y_row[col] = jnp.dot(reduced, inv_ref[...], preferred_element_type=jnp.float32)

    def send_y(i, carry):
        remote(y_row.at[col], y_in.at[own_slot, col], y_send.at[i], y_recv.at[own_slot, col], (i, own_home)).start()
        return carry

    lax.fori_loop(long_first, near_end, send_y, 0)
    for k, peer in enumerate(peers):
        remote(y_row.at[col], y_row.at[col], o_send.at[k], o_recv.at[col], (row, peer)).start()
    pl.when(row == 0)(log_part)
    for k, peer in enumerate(peers):
        remote(logs.at[peer], logs.at[peer], l_send.at[k], l_recv.at[peer], (row, peer)).wait_recv()
        remote(y_row.at[peer], y_row.at[peer], o_send.at[k], o_recv.at[peer], (row, peer)).wait_recv()
    y = y_row[0]
    log_sum = logs[0]
    for s in range(1, n_col):
        y = y + y_row[s]
        log_sum = log_sum + logs[s]
    y_all[...] = y

    def far_copy(i):
        return remote(y_all, y_in.at[own_slot, 0], y_send.at[i], y_recv.at[own_slot, 0], (i, col))

    def send_far(i, carry):
        far_copy(i).start()
        return carry

    lax.fori_loop(jnp.where(relays, near_end, n_row), n_row, send_far, 0)
    white_ref[0, 0] = y
    quadratic = jnp.sum(y * y, axis=1, keepdims=True) * (1.0 / width)
    lik = -0.5 * quadratic + log_sum * (1.0 / width) - 0.5 * math.log(2.0 * math.pi)
    r_id = lax.broadcasted_iota(jnp.int32, (nrhs, 128), 0)
    c_id = lax.broadcasted_iota(jnp.int32, (nrhs, 128), 1)
    flat = jnp.sum(jnp.where(r_id == c_id, lik, 0.0), axis=0, keepdims=True)
    lik_ref[0] = flat[:, :nrhs]

    def left_y(i, carry):
        remote(y_row.at[col], y_in.at[own_slot, col], y_send.at[i], y_recv.at[own_slot, col], (i, own_home)).wait_send()
        return carry

    lax.fori_loop(long_first, near_end, left_y, 0)

    def left_far(i, carry):
        far_copy(i).wait_send()
        return carry

    lax.fori_loop(jnp.where(relays, near_end, n_row), n_row, left_far, 0)
    for k, peer in enumerate(peers):
        remote(logs.at[col], logs.at[col], l_send.at[k], l_recv.at[col], (row, peer)).wait_send()
        remote(y_row.at[col], y_row.at[col], o_send.at[k], o_recv.at[col], (row, peer)).wait_send()

    @pl.when(feeds)
    def _():
        for s in range(n_col):
            remote(w_out, w_in.at[col], w_send.at[s], w_recv.at[col], (row + 1, s)).wait_send()

    @pl.when(gives)
    def _():
        for s in range(n_col):
            part = pl.ds(s, n_col - s)

            @pl.when(by_way(s))
            def _():
                remote(v_out.at[part], v_out.at[part], m_send.at[s], m_recv.at[0], (row, s)).wait_send()

            @pl.when(jnp.logical_not(by_way(s)))
            def _():
                v_copy(s, row - 1).wait_send()

        for k, peer in enumerate(peers):
            u_copy(k, peer).wait_send()

    for cc in range(n_col):
        part = pl.ds(cc, n_col - cc)

        @pl.when(by_way(col) & (col == cc))
        def _():
            remote(v_out.at[part], v_in.at[part], f_send, v_recv, (row - 1, cc)).wait_send()

    for q in range(per_col):
        j = q * n_col + col

        @pl.when(j < long_count)
        def _():
            for k, peer in enumerate(peers):
                remote(p_out.at[q, peer], p_in.at[j], p_send.at[q, k], p_recv.at[j], (row, peer)).wait_send()


def local(n_row, n_col, right_side, inverse_t, u_factor, v_factor, ranks):
    nrhs, width = right_side.shape[2:]
    per_col, _, rank_max = u_factor.shape[2:5]
    piece = width // n_col
    vmem = pl.BlockSpec(memory_space=pltpu.VMEM)
    hbm = pl.BlockSpec(memory_space=pl.ANY)
    dma = pltpu.SemaphoreType.DMA

    def f32(*shape):
        return pltpu.VMEM(shape, jnp.float32)

    def bf16(*shape):
        return pltpu.VMEM(shape, jnp.bfloat16)

    return pl.pallas_call(
        functools.partial(kernel, n_row, n_col),
        out_shape=(
            pltpu.VMEM((1, 1, nrhs, width), jnp.float32),
            pltpu.VMEM((1, 1, nrhs), jnp.float32),
        ),
        in_specs=[hbm, hbm, hbm, hbm, pl.BlockSpec(memory_space=pltpu.SMEM)],
        out_specs=(vmem, vmem),
        scratch_shapes=[
            f32(nrhs, width),
            bf16(piece, width),
            bf16(per_col, rank_max, width),
            bf16(per_col, rank_max, width),
            f32(per_col, n_col, nrhs, width),
            f32(per_col, n_col, nrhs, piece),
            f32(n_row, nrhs, piece),
            f32(n_col, nrhs, width),
            f32(n_col, 1, 128),
            f32(nrhs, piece),
            f32(n_col, rank_max, piece),
            f32(n_col, rank_max, piece),
            f32(n_col, rank_max, piece),
            f32(rank_max, piece),
            f32(piece, rank_max),
            f32(nrhs, rank_max),
            f32(n_col, nrhs, rank_max),
            f32(nrhs, width),
            f32(nrhs, width),
            dma((4,)),
            dma((n_row,)),
            dma((per_col, n_col)),
            dma((per_col, n_col)),
            dma((n_row,)),
            dma((n_col,)),
            dma((n_col,)),
            dma((n_col,)),
            dma((n_col,)),
            dma((n_col,)),
            dma,
            dma((n_col,)),
            dma,
            dma((n_col,)),
            dma((n_col,)),
            dma((n_col,)),
            dma((n_col,)),
            dma,
        ],
        compiler_params=pltpu.CompilerParams(collective_id=0, has_side_effects=True),
        name="forward_solve",
    )(right_side, inverse_t, u_factor, v_factor, ranks.reshape(per_col))


def solution(mesh):
    placed = (
        P(None, "row", None, None),
        P(None, "row", "col", None),
        P(None, "row", None, "col", None, None),
        P(None, "row", None, "col", None, None),
        P(None, "row", None, "col"),
    )
    return jax.shard_map(
        functools.partial(local, mesh.shape["row"], mesh.shape["col"]),
        mesh=mesh,
        in_specs=placed,
        out_specs=(P(None, "row", None, None), P(None, "row", None)),
        check_vma=False,
    )
```
